32 devices in a mesh: grp: 4 (over y, x), dev: 8 (over z, core).
Axes of the slice: x: 2, y: 2, z: 4, core: 2. Of those that a mesh axis runs over, the one named last changes fastest.
Arguments:
- embeddings: bfloat16 [262144, 256], P(('grp', 'dev'))
- prior_dist: float32 [262144], P(('grp', 'dev')), may hold values from 1 to 3
- seed_ids: int32 [6, 512], replicated, may hold values from 0 to 262143, as said below
Outputs:
- min_dist: float32 [262144], P(('grp', 'dev'))
- group_means: float32 [6, 4], P(None, 'grp')
The draws below stay inside these ranges and needn't reach their ends.
Inputs may be any that keep to these rules, and one draw needn't show every extreme that they name: `seed_ids`: round r's ids all lie in the rows of group r mod 4, that is from (r mod 4) * 65536 to (r mod 4 + 1) * 65536 - 1; ids may repeat.
All inputs are finite; a program needn't handle non-finite values.
Results may differ from the reference program's by a relative error of at most 0.0003.
Values may be sent and summed in bfloat16 or wider, within the bound.
No kernel may reach another device: no remote copies, remote signals or barrier semaphores. Data moves between devices by JAX's collectives and lax.ppermute only.
A program may use at most 64 MiB of HBM per device.

```python
import jax
import jax.numpy as jnp
from jax import lax

W = 256
SEEDS = 512
ROUNDS = 6
ROW_DEV = 8192
GROUP_ROWS = 65536
ROWS = 262144
GROUPS = 4


def draw_embeddings(key, part):
    key_rows, key_scale, key_shift, key_center, key_member = jax.random.split(jax.random.fold_in(key, 11), 5)
    cluster_count = 4 * SEEDS
    member = jax.random.randint(key_member, (ROWS,), 0, cluster_count, dtype=jnp.int32)
    centroids = jax.random.normal(key_center, (cluster_count, W), jnp.float32)
    scales = jnp.exp(jax.random.uniform(key_scale, (cluster_count,), jnp.float32, -0.7, 0.7))
    row_scale = jnp.take(scales, member, axis=0)
    row_center = jnp.take(centroids, member, axis=0)
    noise = jax.random.normal(key_rows, (ROWS, W), jnp.float32)
    values = row_scale[:, None] * (row_center + 0.3 * noise)
    return values.astype(jnp.bfloat16)


def draw_seed_ids(key, part):
    owners = jnp.arange(ROUNDS, dtype=jnp.int32) % GROUPS
    within = jax.random.randint(jax.random.fold_in(key, 23), (ROUNDS, SEEDS), 0, GROUP_ROWS, dtype=jnp.int32)
    return (owners[:, None] * GROUP_ROWS + within).astype(jnp.int32)


def steps_of(own_key, extent, cuts, least, top_value):
    factor_of = 1.0
    for position, blocks in cuts:
        steps = jax.random.uniform(jax.random.fold_in(jax.random.fold_in(own_key, 6), position), (blocks,), jnp.float32, least / len(cuts), top_value / len(cuts))
        factor_of = factor_of * jnp.repeat(jnp.exp(steps), extent[position] // blocks).reshape((-1,) + (1,) * (len(extent) - 1 - position))
    return factor_of


def setup_inputs(seed: int = 0) -> dict:
    key_of = jax.random.split(jax.random.key(seed), 4)
    return {
        "embeddings": draw_embeddings(jax.random.fold_in(key_of[3], 71), 0),
        "prior_dist": jnp.clip(1.0 + 2.0 * jax.random.uniform(key_of[1], (ROWS,), jnp.float32) ** steps_of(key_of[1], (ROWS,), ((0, 32),), -0.2, 0.2), 1.0, 3.0),
        "seed_ids": draw_seed_ids(jax.random.fold_in(key_of[3], 71), 0),
    }


def block_nearest(block, block_norms, centers, seed_norms):
    products = jnp.dot(block, centers.T, preferred_element_type=jnp.float32)
    gaps = jnp.maximum(block_norms[:, None] + seed_norms[None, :] - 2.0 * products, 0.0) / float(W)
    return jnp.min(gaps, axis=1)


def reference(embeddings, prior_dist, seed_ids):
    row_norms = jnp.sum(jnp.square(embeddings.astype(jnp.float32)), axis=1)
    block_count = ROWS // ROW_DEV
    blocks = embeddings.reshape(block_count, ROW_DEV, W)
    norm_blocks = row_norms.reshape(block_count, ROW_DEV)
    current = prior_dist
    means = []
    for round_index in range(ROUNDS):
        centers = jnp.take(embeddings, seed_ids[round_index], axis=0)
        seed_norms = jnp.sum(jnp.square(centers.astype(jnp.float32)), axis=1)

        def one_block(pair):
            return block_nearest(pair[0], pair[1], centers, seed_norms)

        nearest = lax.map(one_block, (blocks, norm_blocks)).reshape(ROWS)
        current = jnp.minimum(current, nearest)
        means.append(jnp.sum(current.reshape(GROUPS, GROUP_ROWS), axis=1) / float(GROUP_ROWS))
    return current, jnp.stack(means)
```

```python
import functools

import jax
import jax.numpy as jnp
from jax import lax
from jax.experimental import pallas as pl
from jax.experimental.pallas import tpu as pltpu
from jax.sharding import PartitionSpec as P


NT = (((1,), (1,)), ((), ()))
LANES = 128
BLOCK = 2048
ONCE = pltpu.CompilerParams(dimension_semantics=("arbitrary",))


def pick_kernel(place_ref, source_ref, emb_ref, send_ref, keep_ref, wide_ref, *, steps, step_rows, owned, share, spots):
    step = pl.program_id(0)
    row_count = steps * step_rows
    wide_ref[pl.ds(pl.multiple_of(step * step_rows, step_rows), step_rows), :] = emb_ref[...].astype(jnp.float32)

    @pl.when(step == steps - 1)
    def _():
        wide_ref[pl.ds(row_count, 8), :] = jnp.zeros((8, wide_ref.shape[1]), jnp.float32)
        core = place_ref[0]
        spot = place_ref[1]
        tile = 16
        for half, out_ref in ((1 - core, send_ref), (core, keep_ref)):

            def pick(j, carry, half=half, out_ref=out_ref):
                slot = (half * spots + (spot ^ j)) * share
                for k in range(owned):
                    round_index = place_ref[2 + k]
                    for b in range(0, share, tile):
                        rows = [
                            wide_ref[pl.ds(source_ref[round_index, slot + b + lane], 1), :] for lane in range(tile)
                        ]
                        start = (j * owned + k) * share + b
                        out_ref[pl.ds(pl.multiple_of(start, tile), tile), :] = jnp.concatenate(rows, axis=0).astype(
                            jnp.bfloat16
                        )
                return carry

            lax.fori_loop(0, spots, pick, 0)


def pick_rows(place, sources, embeddings, owned, share, spots):
    row_count, width = embeddings.shape
    steps = 4
    step_rows = row_count // steps
    total = spots * owned * share
    return pl.pallas_call(
        functools.partial(
            pick_kernel, steps=steps, step_rows=step_rows, owned=owned, share=share, spots=spots
        ),
        grid_spec=pltpu.PrefetchScalarGridSpec(
            num_scalar_prefetch=2,
            grid=(steps,),
            in_specs=[pl.BlockSpec((step_rows, width), lambda i, *_: (i, 0))],
            out_specs=[pl.BlockSpec((total, width), lambda i, *_: (0, 0))] * 2,
            scratch_shapes=[pltpu.VMEM((row_count + 8, width), jnp.float32)],
        ),
        out_shape=[jax.ShapeDtypeStruct((total, width), jnp.bfloat16)] * 2,
        compiler_params=ONCE,
        name="pick_rows",
    )(place, sources, embeddings)


def prepare(chunks, refs, norms_ref, minus_ref):
    at = 0
    for chunk in chunks:
        for terms, start, count in chunk:
            wide = refs[terms[0]][pl.ds(start, count), :].astype(jnp.float32)
            for term in terms[1:]:
                wide = wide + refs[term][pl.ds(start, count), :].astype(jnp.float32)
            total = jnp.sum(wide * wide, axis=1, keepdims=True)
            norms_ref[pl.ds(at, count), :] = jnp.broadcast_to(total, (count, LANES))
            minus_ref[pl.ds(at, count), :] = (wide * -2.0).astype(jnp.bfloat16)
            at += count


def norms_of(block):
    wide = block.astype(jnp.float32)
    square = wide * wide
    high = square.astype(jnp.bfloat16)
    low = (square - high.astype(jnp.float32)).astype(jnp.bfloat16)
    ones = jnp.ones((8, block.shape[1]), jnp.bfloat16)
    total = lax.dot_general(ones, high, NT, preferred_element_type=jnp.float32)
    total += lax.dot_general(ones, low, NT, preferred_element_type=jnp.float32)
    return total[:1]


def block_gaps(index, seeds, rows, row_norms, norms_ref, minus_ref):
    products = lax.dot_general(
        minus_ref[pl.ds(index * seeds, seeds), :], rows, NT, preferred_element_type=jnp.float32
    )
    norms = norms_ref[pl.ds(index * seeds, seeds), :]
    parts = [
        jnp.min(products[:, start : start + LANES] + norms, axis=0, keepdims=True)
        for start in range(0, rows.shape[0], LANES)
    ]
    return jnp.maximum(row_norms + jnp.concatenate(parts, axis=1), 0.0) * (1.0 / rows.shape[1])


def near_kernel(*refs, chunks, arrays, seeds, opening):
    seeds_refs, rest = refs[:arrays], refs[arrays:]
    if opening:
        rows_ref, near_ref, row_norms_ref, norms_ref, minus_ref = rest
    else:
        rows_ref, row_norms_ref, near_ref, norms_ref, minus_ref = rest

    @pl.when(pl.program_id(0) == 0)
    def _():
        prepare(chunks, seeds_refs, norms_ref, minus_ref)

    rows = rows_ref[...]
    if opening:
        row_norms = norms_of(rows)
        row_norms_ref[...] = row_norms
    else:
        row_norms = row_norms_ref[...]
    for index in range(len(chunks)):
        near_ref[index] = block_gaps(index, seeds, rows, row_norms, norms_ref, minus_ref)


def last_kernel(place_ref, *refs, chunks, arrays, seeds, first, olds):
    seeds_refs, rest = refs[:arrays], refs[arrays:]
    rows_ref, row_norms_ref, prior_ref = rest[:3]
    old_refs = rest[3 : 3 + olds]
    dist_ref, sums_ref, norms_ref, minus_ref, near_ref, add_ref = rest[3 + olds :]
    rounds = near_ref.shape[0]

    @pl.when(pl.program_id(0) == 0)
    def _():
        add_ref[...] = jnp.zeros_like(add_ref)
        prepare(chunks, seeds_refs, norms_ref, minus_ref)

    rows = rows_ref[...]
    row_norms = row_norms_ref[...]
    place = 0
    for old_ref in old_refs:
        for index in range(old_ref.shape[0]):
            near_ref[place_ref[first + place]] = old_ref[index]
            place += 1
    for index in range(len(chunks)):
        near_ref[place_ref[first + place]] = block_gaps(index, seeds, rows, row_norms, norms_ref, minus_ref)
        place += 1
    current = prior_ref[...]
    for index in range(rounds):
        current = jnp.minimum(current, near_ref[index])
        folded = current[:, :LANES]
        for start in range(LANES, rows.shape[0], LANES):
            folded = folded + current[:, start : start + LANES]
        add_ref[pl.ds(index, 1), :] += folded
    dist_ref[...] = current

    @pl.when(pl.program_id(0) == pl.num_programs(0) - 1)
    def _():
        total = jnp.sum(add_ref[...], axis=1, keepdims=True)
        sums_ref[...] = jnp.broadcast_to(total, sums_ref.shape)


def near_rows(chunks, pool, embeddings, row_norms, seeds, place=None, first=0, prior=None, olds=None, rounds=0):
    row_count, width = embeddings.shape
    rows = min(BLOCK, row_count)
    used = sorted({term for chunk in chunks for terms, _, _ in chunk for term in terms})
    arrays = [pool[term] for term in used]
    chunks = tuple(
        tuple((tuple(used.index(term) for term in terms), start, count) for terms, start, count in chunk)
        for chunk in chunks
    )
    count = len(chunks)
    grid = (row_count // rows,)
    whole = [pl.BlockSpec(array.shape, lambda i, *_: (0, 0)) for array in arrays]
    flat = pl.BlockSpec((1, rows), lambda i, *_: (0, i))
    tall = pl.BlockSpec((rows, width), lambda i, *_: (i, 0))
    flat_shape = jax.ShapeDtypeStruct((1, row_count), jnp.float32)
    scratch = [
        pltpu.VMEM((count * seeds, LANES), jnp.float32),
        pltpu.VMEM((count * seeds, width), jnp.bfloat16),
    ]
    common = dict(chunks=chunks, arrays=len(arrays), seeds=seeds)
    if olds is None:
        opening = row_norms is None
        near_spec = pl.BlockSpec((count, 1, rows), lambda i: (0, 0, i))
        near_shape = jax.ShapeDtypeStruct((count, 1, row_count), jnp.float32)
        return pl.pallas_call(
            functools.partial(near_kernel, opening=opening, **common),
            grid=grid,
            in_specs=whole + [tall] + ([] if opening else [flat]),
            out_specs=[near_spec, flat] if opening else near_spec,
            out_shape=[near_shape, flat_shape] if opening else near_shape,
            scratch_shapes=scratch,
            compiler_params=ONCE,
            name="near_rows",
        )(*arrays, embeddings, *([] if opening else [row_norms]))
    padded = -(-rounds // 8) * 8
    return pl.pallas_call(
        functools.partial(last_kernel, first=first, olds=len(olds), **common),
        grid_spec=pltpu.PrefetchScalarGridSpec(
            num_scalar_prefetch=1,
            grid=grid,
            in_specs=whole
            + [tall, flat, flat]
            + [pl.BlockSpec((old.shape[0], 1, rows), lambda i, *_: (0, 0, i)) for old in olds],
            out_specs=[flat, pl.BlockSpec((padded, LANES), lambda i, *_: (0, 0))],
            scratch_shapes=scratch
            + [pltpu.VMEM((rounds, 1, rows), jnp.float32), pltpu.VMEM((padded, LANES), jnp.float32)],
        ),
        out_shape=[flat_shape, jax.ShapeDtypeStruct((padded, LANES), jnp.float32)],
        compiler_params=ONCE,
        name="last_rows",
    )(place, *arrays, embeddings, row_norms, prior, *olds)


def tree_sum(items):
    while len(items) > 1:
        items = [items[i] + items[i + 1] for i in range(0, len(items), 2)]
    return items[0]


def body(embeddings, prior_dist, seed_ids):
    row_count, width = embeddings.shape
    rounds, seeds = seed_ids.shape
    devs = lax.axis_size("dev")
    groups = lax.axis_size("grp")
    group = lax.axis_index("grp")
    dev = lax.axis_index("dev")
    owned = -(-rounds // groups)
    full = rounds // groups
    extra = rounds % groups
    spots = devs // 2
    share = seeds // devs

    def swap(array, axis, bits, size):
        return lax.ppermute(array, axis, [(i, i ^ bits) for i in range(size)])

    stages = [[0], list(range(1, groups - 1)), [groups - 1]]
    plan, labels = [], []

    def chunk_of(hops, k):
        return tuple(
            (tuple(2 * j + side for j in hops), (p * owned + k) * share, share)
            for side in range(2)
            for p in range(spots)
        )

    for stage in stages:
        chunks = []
        for j in stage:
            for k in range(full):
                chunks.append(chunk_of([j], k))
                labels.append(k * groups + (group ^ j))
        for i in range(extra):
            hops = [j for j in range(groups) if j % extra == i]
            if max(hops) in stage:
                chunks.append(chunk_of(hops, full))
                labels.append(full * groups + ((group % extra) ^ i))
        plan.append(chunks)

    owned_rounds = [jnp.minimum(group + k * groups, rounds - 1) for k in range(owned)]
    place = jnp.stack([dev % 2, dev // 2] + owned_rounds + labels).astype(jnp.int32)
    first = 2 + owned
    offsets = seed_ids - (group * devs + dev) * row_count
    sources = jnp.where((offsets >= 0) & (offsets < row_count), offsets, row_count)

    send, keep = pick_rows(place, sources, embeddings, owned, share, spots)
    mine = (keep + swap(send, "dev", 1, devs)).reshape(spots, owned * share, width)
    piece = tree_sum([mine[0]] + [swap(mine[j], "dev", 2 * j, devs) for j in range(1, spots)])
    column = jnp.concatenate([piece] + [swap(piece, "dev", 2 * j, devs) for j in range(1, spots)], axis=0)
    pool = []
    for j in range(groups):
        own = column if j == 0 else swap(column, "grp", j, groups)
        pool += [own, swap(own, "dev", 1, devs)]

    near, row_norms = near_rows(plan[0], pool, embeddings, None, seeds)
    olds = [near]
    for chunks in plan[1:-1]:
        olds.append(near_rows(chunks, pool, embeddings, row_norms, seeds))
    dist, sums = near_rows(
        plan[-1], pool, embeddings, row_norms, seeds, place, first, prior_dist.reshape(1, row_count), olds, rounds
    )
    pair = sums + swap(sums, "dev", 1, devs)
    means = tree_sum([pair] + [swap(pair, "dev", 2 * j, devs) for j in range(1, spots)])
    means = means[:rounds, :1] / float(row_count * devs)
    return dist.reshape(row_count), means


def solution(mesh):
    placed = (P(("grp", "dev"), None), P(("grp", "dev")), P())
    return jax.shard_map(
        body,
        mesh=mesh,
        in_specs=placed,
        out_specs=(P(("grp", "dev")), P(None, "grp")),
        check_vma=False,
    )
```

```python
import functools

import jax
import jax.numpy as jnp
from jax import lax
from jax.experimental import pallas as pl
from jax.experimental.pallas import tpu as pltpu
from jax.sharding import PartitionSpec as P


NT = (((1,), (1,)), ((), ()))
LANES = 128
BLOCK = 2048
COLUMNS = 512
ONCE = pltpu.CompilerParams(dimension_semantics=("arbitrary",), vmem_limit_bytes=32 * 1024 * 1024)


def pick_kernel(ids_ref, emb_ref, send_ref, keep_ref, *wide_refs, steps, step_rows, share, spots):
    step = pl.program_id(0)
    row_count = steps * step_rows
    rows = emb_ref[...].astype(jnp.float32)
    for part, wide_ref in enumerate(wide_refs):
        at = pl.ds(pl.multiple_of(step * step_rows, step_rows), step_rows)
        wide_ref[at, :] = rows[:, part * LANES : (part + 1) * LANES]

    @pl.when(step == steps - 1)
    def _():
        for wide_ref in wide_refs:
            wide_ref[pl.ds(row_count, 8), :] = jnp.zeros((8, LANES), jnp.float32)
        rounds = ids_ref.shape[0]
        groups = lax.axis_size("grp")
        group = lax.axis_index("grp")
        dev = lax.axis_index("dev")
        row_start = (group * lax.axis_size("dev") + dev) * row_count
        core = dev % 2
        spot = dev // 2
        owned = -(-rounds // groups)
        tile = 16
        for half, out_ref in ((1 - core, send_ref), (core, keep_ref)):

            def pick(j, carry, half=half, out_ref=out_ref):
                slot = (half * spots + (spot ^ j)) * share
                for k in range(owned):
                    round_index = jnp.minimum(group + k * groups, rounds - 1)
                    for b in range(0, share, tile):
                        found = []
                        for lane in range(tile):
                            offset = ids_ref[round_index, slot + b + lane] - row_start
                            inside = offset.astype(jnp.uint32) < jnp.uint32(row_count)
                            found.append(jnp.where(inside, offset, row_count))
                        start = pl.multiple_of((j * owned + k) * share + b, tile)
                        for part, wide_ref in enumerate(wide_refs):
                            picked = [wide_ref[pl.ds(source, 1), :] for source in found]
                            out_ref[pl.ds(start, tile), part * LANES : (part + 1) * LANES] = jnp.concatenate(
                                picked, axis=0
                            ).astype(jnp.bfloat16)
                return carry

            lax.fori_loop(0, spots, pick, 0)


def pick_rows(seed_ids, embeddings, owned, share, spots):
    row_count, width = embeddings.shape
    steps = 4
    step_rows = row_count // steps
    total = spots * owned * share
    return pl.pallas_call(
        functools.partial(pick_kernel, steps=steps, step_rows=step_rows, share=share, spots=spots),
        grid_spec=pltpu.PrefetchScalarGridSpec(
            num_scalar_prefetch=1,
            grid=(steps,),
            in_specs=[pl.BlockSpec((step_rows, width), lambda i, *_: (i, 0))],
            out_specs=[pl.BlockSpec((total, width), lambda i, *_: (0, 0))] * 2,
            scratch_shapes=[pltpu.VMEM((row_count + 8, LANES), jnp.float32)] * (width // LANES),
        ),
        out_shape=[jax.ShapeDtypeStruct((total, width), jnp.bfloat16)] * 2,
        compiler_params=ONCE,
        name="pick_rows",
    )(seed_ids, embeddings)


def fast(array):
    return pltpu.with_memory_space_constraint(array, pltpu.VMEM)


def prepare(chunks, refs, norms_ref, minus_ref):
    at = 0
    for chunk in chunks:
        for terms, start, count in chunk:
            wide = refs[terms[0]][pl.ds(start, count), :].astype(jnp.float32)
            for term in terms[1:]:
                wide = wide + refs[term][pl.ds(start, count), :].astype(jnp.float32)
            total = jnp.sum(wide * wide, axis=1, keepdims=True)
            norms_ref[pl.ds(at, count), :] = jnp.broadcast_to(total, (count, LANES))
            minus_ref[pl.ds(at, count), :] = (wide * -2.0).astype(jnp.bfloat16)
            at += count


def norms_of(block):
    wide = block.astype(jnp.float32)
    square = wide * wide
    high = square.astype(jnp.bfloat16)
    low = (square - high.astype(jnp.float32)).astype(jnp.bfloat16)
    ones = jnp.ones((8, block.shape[1]), jnp.bfloat16)
    total = lax.dot_general(ones, high, NT, preferred_element_type=jnp.float32)
    total += lax.dot_general(ones, low, NT, preferred_element_type=jnp.float32)
    return total[:1]


def block_gaps(sizes, rows, row_norms, norms_ref, minus_ref):
    nearest = [[] for _ in sizes]
    for left in range(0, rows.shape[0], COLUMNS):
        products = lax.dot_general(
            minus_ref[...], rows[left : left + COLUMNS], NT, preferred_element_type=jnp.float32
        )
        for start in range(0, COLUMNS, LANES):
            at = 0
            for index, size in enumerate(sizes):
                part = products[at : at + size, start : start + LANES] + norms_ref[pl.ds(at, size), :]
                nearest[index].append(jnp.min(part, axis=0, keepdims=True))
                at += size
    return [
        jnp.maximum(row_norms + jnp.concatenate(parts, axis=1), 0.0) * (1.0 / rows.shape[1]) for parts in nearest
    ]


def near_kernel(*refs, chunks, sizes, arrays, opening):
    seeds_refs, rest = refs[:arrays], refs[arrays:]
    if opening:
        rows_ref, near_ref, row_norms_ref, norms_ref, minus_ref = rest
    else:
        rows_ref, row_norms_ref, near_ref, norms_ref, minus_ref = rest

    @pl.when(pl.program_id(0) == 0)
    def _():
        prepare(chunks, seeds_refs, norms_ref, minus_ref)

    rows = rows_ref[pl.ds(pl.multiple_of(pl.program_id(0) * BLOCK, BLOCK), BLOCK), :]
    if opening:
        row_norms = norms_of(rows)
        row_norms_ref[...] = row_norms
    else:
        row_norms = row_norms_ref[...]
    for index, gaps in enumerate(block_gaps(sizes, rows, row_norms, norms_ref, minus_ref)):
        near_ref[index] = gaps


def last_kernel(*refs, chunks, sizes, arrays, olds, labels):
    seeds_refs, rest = refs[:arrays], refs[arrays:]
    rows_ref, row_norms_ref, prior_ref = rest[:3]
    old_refs = rest[3 : 3 + olds]
    dist_ref, sums_ref, norms_ref, minus_ref, near_ref, add_ref = rest[3 + olds :]
    rounds = near_ref.shape[0]

    @pl.when(pl.program_id(0) == 0)
    def _():
        add_ref[...] = jnp.zeros_like(add_ref)
        prepare(chunks, seeds_refs, norms_ref, minus_ref)

    rows = rows_ref[pl.ds(pl.multiple_of(pl.program_id(0) * BLOCK, BLOCK), BLOCK), :]
    row_norms = row_norms_ref[...]
    group = lax.axis_index("grp")
    current = prior_ref[...]
    for index in range(rounds):
        near_ref[index] = current
    gaps = [old_ref[index] for old_ref in old_refs for index in range(old_ref.shape[0])]
    gaps += block_gaps(sizes, rows, row_norms, norms_ref, minus_ref)
    for (base, period, bits), gap in zip(labels, gaps):
        label = base + ((group % period) ^ bits)
        near_ref[label] = jnp.minimum(near_ref[label], gap)
    for index in range(rounds):
        current = jnp.minimum(current, near_ref[index])
        folded = current[:, :LANES]
        for start in range(LANES, rows.shape[0], LANES):
            folded = folded + current[:, start : start + LANES]
        add_ref[pl.ds(index, 1), :] += folded
    dist_ref[...] = current

    @pl.when(pl.program_id(0) == pl.num_programs(0) - 1)
    def _():
        total = jnp.sum(add_ref[...], axis=1, keepdims=True)
        sums_ref[...] = jnp.broadcast_to(total, sums_ref.shape)


def near_rows(chunks, pool, embeddings, row_norms, prior=None, olds=None, labels=(), rounds=0):
    row_count, width = embeddings.shape
    rows = min(BLOCK, row_count)
    used = sorted({term for chunk in chunks for terms, _, _ in chunk for term in terms})
    arrays = [pool[term] for term in used]
    chunks = tuple(
        tuple((tuple(used.index(term) for term in terms), start, count) for terms, start, count in chunk)
        for chunk in chunks
    )
    count = len(chunks)
    sizes = tuple(sum(piece[2] for piece in chunk) for chunk in chunks)
    grid = (row_count // rows,)
    arrays = [fast(array) for array in arrays]
    whole = [pl.BlockSpec(memory_space=pltpu.VMEM) for array in arrays]
    flat = pl.BlockSpec((1, rows), lambda i, *_: (0, i))
    tall = pl.BlockSpec(memory_space=pltpu.VMEM)
    flat_shape = jax.ShapeDtypeStruct((1, row_count), jnp.float32)
    scratch = [
        pltpu.VMEM((sum(sizes), LANES), jnp.float32),
        pltpu.VMEM((sum(sizes), width), jnp.bfloat16),
    ]
    common = dict(chunks=chunks, sizes=sizes, arrays=len(arrays))
    if olds is None:
        opening = row_norms is None
        near_spec = pl.BlockSpec((count, 1, rows), lambda i: (0, 0, i))
        near_shape = jax.ShapeDtypeStruct((count, 1, row_count), jnp.float32)
        return pl.pallas_call(
            functools.partial(near_kernel, opening=opening, **common),
            grid=grid,
            in_specs=whole + [tall] + ([] if opening else [flat]),
            out_specs=[near_spec, flat] if opening else near_spec,
            out_shape=[near_shape, flat_shape] if opening else near_shape,
            scratch_shapes=scratch,
            compiler_params=ONCE,
            name="near_rows",
        )(*arrays, embeddings, *([] if opening else [row_norms]))
    padded = -(-rounds // 8) * 8
    return pl.pallas_call(
        functools.partial(last_kernel, olds=len(olds), labels=labels, **common),
        grid=grid,
        in_specs=whole
        + [tall, flat, flat]
        + [pl.BlockSpec((old.shape[0], 1, rows), lambda i: (0, 0, i)) for old in olds],
        out_specs=[flat, pl.BlockSpec((padded, LANES), lambda i: (0, 0))],
        scratch_shapes=scratch
        + [pltpu.VMEM((rounds, 1, rows), jnp.float32), pltpu.VMEM((padded, LANES), jnp.float32)],
        out_shape=[flat_shape, jax.ShapeDtypeStruct((padded, LANES), jnp.float32)],
        compiler_params=ONCE,
        name="last_rows",
    )(*arrays, embeddings, row_norms, prior, *olds)


def tree_sum(items):
    while len(items) > 1:
        items = [items[i] + items[i + 1] for i in range(0, len(items), 2)]
    return items[0]


def body(embeddings, prior_dist, seed_ids):
    row_count, width = embeddings.shape
    rounds, seeds = seed_ids.shape
    devs = lax.axis_size("dev")
    groups = lax.axis_size("grp")
    owned = -(-rounds // groups)
    full = rounds // groups
    extra = rounds % groups
    spots = devs // 2
    share = seeds // devs

    def swap(array, axis, bits, size):
        return lax.ppermute(array, axis, [(i, i ^ bits) for i in range(size)])

    def plan(distances, sides):
        chunks, labels = [], []

        def add(hops, k, label):
            chunks.append(
                tuple(
                    (tuple(2 * j + side for j in hops), (p * owned + k) * share, share)
                    for side in sides
                    for p in range(spots)
                )
            )
            labels.append(label)

        for j in distances:
            for k in range(full):
                add([j], k, (k * groups, groups, j))
        for i in range(extra if max(distances) else 0):
            add([j for j in range(groups) if j % extra == i], full, (full * groups, extra, i))
        return chunks, labels

    send, keep = pick_rows(seed_ids, embeddings, owned, share, spots)
    mine = (keep + swap(send, "dev", 1, devs)).reshape(spots, owned * share, width)
    piece = tree_sum([mine[0]] + [swap(mine[j], "dev", 2 * j, devs) for j in range(1, spots)])
    column = jnp.concatenate([piece] + [swap(piece, "dev", 2 * j, devs) for j in range(1, spots)], axis=0)

    resident = fast(embeddings)
    pool = {0: column, 1: swap(column, "dev", 1, devs)}
    far = [swap(column, "grp", j, groups) for j in range(1, groups)]
    chunks, labels = plan([0], [0, 1])
    near, row_norms = near_rows(chunks, pool, resident, None)
    olds = [near]
    far, row_norms = lax.optimization_barrier((far, row_norms))
    for j in range(1, groups):
        pool[2 * j] = far[j - 1]
        pool[2 * j + 1] = swap(far[j - 1], "dev", 1, devs)
    chunks, more = plan(range(1, groups), [0])
    labels += more
    olds.append(near_rows(chunks, pool, resident, row_norms))
    chunks, more = plan(range(1, groups), [1])
    labels += more
    dist, sums = near_rows(
        chunks, pool, embeddings, row_norms, prior_dist.reshape(1, row_count), olds, tuple(labels), rounds
    )
    pair = sums + swap(sums, "dev", 1, devs)
    means = tree_sum([pair] + [swap(pair, "dev", 2 * j, devs) for j in range(1, spots)])
    means = means[:rounds, :1] / float(row_count * devs)
    return dist.reshape(row_count), means


def solution(mesh):
    placed = (P(("grp", "dev"), None), P(("grp", "dev")), P())
    return jax.shard_map(
        body,
        mesh=mesh,
        in_specs=placed,
        out_specs=(P(("grp", "dev")), P(None, "grp")),
        check_vma=False,
    )
```

```python
import functools

import jax
import jax.numpy as jnp
from jax import lax
from jax.experimental import pallas as pl
from jax.experimental.pallas import tpu as pltpu
from jax.sharding import PartitionSpec as P


NT = (((1,), (1,)), ((), ()))
LANES = 128
BLOCK = 2048
COLUMNS = 512
ONCE = pltpu.CompilerParams(dimension_semantics=("arbitrary",), vmem_limit_bytes=32 * 1024 * 1024)


def pick_kernel(ids_ref, emb_ref, send_ref, keep_ref, *wide_refs, steps, step_rows, share, spots):
    step = pl.program_id(0)
    row_count = steps * step_rows
    rows = emb_ref[...].astype(jnp.float32)
    for part, wide_ref in enumerate(wide_refs):
        at = pl.ds(pl.multiple_of(step * step_rows, step_rows), step_rows)
        wide_ref[at, :] = rows[:, part * LANES : (part + 1) * LANES]

    @pl.when(step == steps - 1)
    def _():
        for wide_ref in wide_refs:
            wide_ref[pl.ds(row_count, 8), :] = jnp.zeros((8, LANES), jnp.float32)
        rounds = ids_ref.shape[0]
        groups = lax.axis_size("grp")
        group = lax.axis_index("grp")
        dev = lax.axis_index("dev")
        row_start = (group * lax.axis_size("dev") + dev) * row_count
        core = dev % 2
        spot = dev // 2
        owned = -(-rounds // groups)
        tile = 16
        for half, out_ref in ((1 - core, send_ref), (core, keep_ref)):

            def pick(j, carry, half=half, out_ref=out_ref):
                slot = (half * spots + (spot ^ j)) * share
                for k in range(owned):
                    round_index = jnp.minimum(group + k * groups, rounds - 1)
                    for b in range(0, share, tile):
                        found = []
                        for lane in range(tile):
                            offset = ids_ref[round_index, slot + b + lane] - row_start
                            inside = offset.astype(jnp.uint32) < jnp.uint32(row_count)
                            found.append(jnp.where(inside, offset, row_count))
                        start = pl.multiple_of((j * owned + k) * share + b, tile)
                        for part, wide_ref in enumerate(wide_refs):
                            picked = [wide_ref[pl.ds(source, 1), :] for source in found]
                            out_ref[pl.ds(start, tile), part * LANES : (part + 1) * LANES] = jnp.concatenate(
                                picked, axis=0
                            ).astype(jnp.bfloat16)
                return carry

            lax.fori_loop(0, spots, pick, 0)


def pick_rows(seed_ids, embeddings, owned, share, spots):
    row_count, width = embeddings.shape
    steps = 4
    step_rows = row_count // steps
    total = spots * owned * share
    return pl.pallas_call(
        functools.partial(pick_kernel, steps=steps, step_rows=step_rows, share=share, spots=spots),
        grid_spec=pltpu.PrefetchScalarGridSpec(
            num_scalar_prefetch=1,
            grid=(steps,),
            in_specs=[pl.BlockSpec((step_rows, width), lambda i, *_: (i, 0))],
            out_specs=[pl.BlockSpec((total, width), lambda i, *_: (0, 0))] * 2,
            scratch_shapes=[pltpu.VMEM((row_count + 8, LANES), jnp.float32)] * (width // LANES),
        ),
        out_shape=[jax.ShapeDtypeStruct((total, width), jnp.bfloat16)] * 2,
        compiler_params=ONCE,
        name="pick_rows",
    )(seed_ids, embeddings)


def fast(array):
    return pltpu.with_memory_space_constraint(array, pltpu.VMEM)


def prepare(chunks, refs, norms_ref, minus_ref):
    at = 0
    for chunk in chunks:
        for term, start, count in chunk:
            wide = refs[term][pl.ds(start, count), :].astype(jnp.float32)
            total = jnp.sum(wide * wide, axis=1, keepdims=True)
            norms_ref[pl.ds(at, count), :] = jnp.broadcast_to(total, (count, LANES))
            minus_ref[pl.ds(at, count), :] = (wide * -2.0).astype(jnp.bfloat16)
            at += count


def norms_of(block):
    wide = block.astype(jnp.float32)
    square = wide * wide
    high = square.astype(jnp.bfloat16)
    low = (square - high.astype(jnp.float32)).astype(jnp.bfloat16)
    ones = jnp.ones((8, block.shape[1]), jnp.bfloat16)
    total = lax.dot_general(ones, high, NT, preferred_element_type=jnp.float32)
    total += lax.dot_general(ones, low, NT, preferred_element_type=jnp.float32)
    return total[:1]


def block_gaps(sizes, rows, row_norms, norms_ref, minus_ref):
    nearest = [[] for _ in sizes]
    for left in range(0, rows.shape[0], COLUMNS):
        products = lax.dot_general(
            minus_ref[...], rows[left : left + COLUMNS], NT, preferred_element_type=jnp.float32
        )
        for start in range(0, COLUMNS, LANES):
            at = 0
            for index, size in enumerate(sizes):
                part = products[at : at + size, start : start + LANES] + norms_ref[pl.ds(at, size), :]
                nearest[index].append(jnp.min(part, axis=0, keepdims=True))
                at += size
    return [
        jnp.maximum(row_norms + jnp.concatenate(parts, axis=1), 0.0) * (1.0 / rows.shape[1]) for parts in nearest
    ]


def near_kernel(*refs, chunks, sizes, arrays, opening):
    seeds_refs, rest = refs[:arrays], refs[arrays:]
    if opening:
        rows_ref, near_ref, row_norms_ref, norms_ref, minus_ref = rest
    else:
        rows_ref, row_norms_ref, near_ref, norms_ref, minus_ref = rest

    @pl.when(pl.program_id(0) == 0)
    def _():
        prepare(chunks, seeds_refs, norms_ref, minus_ref)

    rows = rows_ref[pl.ds(pl.multiple_of(pl.program_id(0) * BLOCK, BLOCK), BLOCK), :]
    if opening:
        row_norms = norms_of(rows)
        row_norms_ref[...] = row_norms
    else:
        row_norms = row_norms_ref[...]
    for index, gaps in enumerate(block_gaps(sizes, rows, row_norms, norms_ref, minus_ref)):
        near_ref[index] = gaps


def last_kernel(*refs, chunks, sizes, arrays, olds, labels):
    seeds_refs, rest = refs[:arrays], refs[arrays:]
    rows_ref, row_norms_ref, prior_ref = rest[:3]
    old_refs = rest[3 : 3 + olds]
    dist_ref, sums_ref, norms_ref, minus_ref, near_ref, add_ref = rest[3 + olds :]
    rounds = near_ref.shape[0]

    @pl.when(pl.program_id(0) == 0)
    def _():
        add_ref[...] = jnp.zeros_like(add_ref)
        prepare(chunks, seeds_refs, norms_ref, minus_ref)

    rows = rows_ref[pl.ds(pl.multiple_of(pl.program_id(0) * BLOCK, BLOCK), BLOCK), :]
    row_norms = row_norms_ref[...]
    group = lax.axis_index("grp")
    current = prior_ref[...]
    for index in range(rounds):
        near_ref[index] = current
    gaps = [old_ref[index] for old_ref in old_refs for index in range(old_ref.shape[0])]
    gaps += block_gaps(sizes, rows, row_norms, norms_ref, minus_ref)
    for (base, period, bits), gap in zip(labels, gaps):
        label = base + ((group % period) ^ bits)
        near_ref[label] = jnp.minimum(near_ref[label], gap)
    for index in range(rounds):
        current = jnp.minimum(current, near_ref[index])
        folded = current[:, :LANES]
        for start in range(LANES, rows.shape[0], LANES):
            folded = folded + current[:, start : start + LANES]
        add_ref[pl.ds(index, 1), :] += folded
    dist_ref[...] = current

    @pl.when(pl.program_id(0) == pl.num_programs(0) - 1)
    def _():
        total = jnp.sum(add_ref[...], axis=1, keepdims=True)
        sums_ref[...] = jnp.broadcast_to(total, sums_ref.shape)


def near_rows(chunks, pool, embeddings, row_norms, prior=None, olds=None, labels=(), rounds=0):
    row_count, width = embeddings.shape
    rows = min(BLOCK, row_count)
    used = sorted({term for chunk in chunks for term, _, _ in chunk})
    arrays = [pool[term] for term in used]
    chunks = tuple(
        tuple((used.index(term), start, count) for term, start, count in chunk) for chunk in chunks
    )
    count = len(chunks)
    sizes = tuple(sum(piece[2] for piece in chunk) for chunk in chunks)
    grid = (row_count // rows,)
    arrays = [fast(array) for array in arrays]
    whole = [pl.BlockSpec(memory_space=pltpu.VMEM) for array in arrays]
    flat = pl.BlockSpec((1, rows), lambda i, *_: (0, i))
    tall = pl.BlockSpec(memory_space=pltpu.VMEM)
    flat_shape = jax.ShapeDtypeStruct((1, row_count), jnp.float32)
    scratch = [
        pltpu.VMEM((sum(sizes), LANES), jnp.float32),
        pltpu.VMEM((sum(sizes), width), jnp.bfloat16),
    ]
    common = dict(chunks=chunks, sizes=sizes, arrays=len(arrays))
    if olds is None:
        opening = row_norms is None
        near_spec = pl.BlockSpec((count, 1, rows), lambda i: (0, 0, i))
        near_shape = jax.ShapeDtypeStruct((count, 1, row_count), jnp.float32)
        return pl.pallas_call(
            functools.partial(near_kernel, opening=opening, **common),
            grid=grid,
            in_specs=whole + [tall] + ([] if opening else [flat]),
            out_specs=[near_spec, flat] if opening else near_spec,
            out_shape=[near_shape, flat_shape] if opening else near_shape,
            scratch_shapes=scratch,
            compiler_params=ONCE,
            name="near_rows",
        )(*arrays, embeddings, *([] if opening else [row_norms]))
    padded = -(-rounds // 8) * 8
    return pl.pallas_call(
        functools.partial(last_kernel, olds=len(olds), labels=labels, **common),
        grid=grid,
        in_specs=whole
        + [tall, flat, flat]
        + [pl.BlockSpec((old.shape[0], 1, rows), lambda i: (0, 0, i)) for old in olds],
        out_specs=[flat, pl.BlockSpec((padded, LANES), lambda i: (0, 0))],
        scratch_shapes=scratch
        + [pltpu.VMEM((rounds, 1, rows), jnp.float32), pltpu.VMEM((padded, LANES), jnp.float32)],
        out_shape=[flat_shape, jax.ShapeDtypeStruct((padded, LANES), jnp.float32)],
        compiler_params=ONCE,
        name="last_rows",
    )(*arrays, embeddings, row_norms, prior, *olds)


def tree_sum(items):
    while len(items) > 1:
        items = [items[i] + items[i + 1] for i in range(0, len(items), 2)]
    return items[0]


def body(embeddings, prior_dist, seed_ids):
    row_count, width = embeddings.shape
    rounds, seeds = seed_ids.shape
    devs = lax.axis_size("dev")
    groups = lax.axis_size("grp")
    owned = -(-rounds // groups)
    full = rounds // groups
    extra = rounds % groups
    spots = devs // 2
    share = seeds // devs

    def swap(array, axis, bits, size, senders=None):
        return lax.ppermute(array, axis, [(i, i ^ bits) for i in range(senders or size)])

    pool, labels, olds = {}, [], []

    def halves(names, sides):
        return [tuple(((name, side), 0, pool[name, side].shape[0]) for side in sides) for name in names]

    send, keep = pick_rows(seed_ids, embeddings, owned, share, spots)
    mine = (keep + swap(send, "dev", 1, devs)).reshape(spots, owned * share, width)
    piece = tree_sum([mine[0]] + [swap(mine[j], "dev", 2 * j, devs) for j in range(1, spots)])
    parts = [piece] + [swap(piece, "dev", 2 * j, devs) for j in range(1, spots)]
    columns = [jnp.concatenate([part[k * share : (k + 1) * share] for part in parts], axis=0) for k in range(owned)]

    def put(name, array):
        pool[name, 0] = array
        pool[name, 1] = swap(array, "dev", 1, devs)

    resident = fast(embeddings)
    own_names = [(k, 0) for k in range(full)]
    far_names = [(k, j) for j in range(1, groups) for k in range(full)]
    for k in range(full):
        put((k, 0), columns[k])
    far = [swap(columns[k], "grp", j, groups) for k, j in far_names]
    near, row_norms = near_rows(halves(own_names, [0, 1]), pool, resident, None)
    olds.append(near)
    columns, far, row_norms = lax.optimization_barrier((columns, far, row_norms))
    late = [swap(columns[full], "grp", j, groups) for j in range(1, groups)] if extra else []
    for name, array in zip(far_names, far):
        put(name, array)
    if not extra:
        olds.append(near_rows(halves(far_names, [0]), pool, resident, row_norms))
    for names in (own_names, far_names) if extra else (own_names, far_names, far_names):
        labels += [(k * groups, groups, j) for k, j in names]
    last = halves(far_names, [0, 1] if extra else [1])
    if extra:
        olds.append(near_rows(last, pool, resident, row_norms))
        late, row_norms, olds = lax.optimization_barrier((late, row_norms, olds))
        late = [columns[full]] + late
        late_names = [(full, i) for i in range(extra)]
        for k, i in late_names:
            put((k, i), tree_sum([late[j] for j in range(groups) if j % extra == i]))
        labels += [(full * groups, extra, i) for _, i in late_names]
        last = halves(late_names, [0, 1])
    dist, sums = near_rows(last, pool, resident, row_norms, prior_dist.reshape(1, row_count), olds, tuple(labels), rounds)
    pair = sums + swap(sums, "dev", 1, devs)
    means = tree_sum([pair] + [swap(pair, "dev", 2 * j, devs) for j in range(1, spots)])
    means = means[:rounds, :1] / float(row_count * devs)
    return dist.reshape(row_count), means


def solution(mesh):
    placed = (P(("grp", "dev"), None), P(("grp", "dev")), P())
    return jax.shard_map(
        body,
        mesh=mesh,
        in_specs=placed,
        out_specs=(P(("grp", "dev")), P(None, "grp")),
        check_vma=False,
    )
```
